256 devices in a mesh: member: 8 (over y, x_lo), space: 32 (over z, x_hi, core).
Axes of the slice: x: 4 (x_hi: 2, x_lo: 2; x = x_hi * 2 + x_lo), y: 4, z: 8, core: 2. Of those that a mesh axis runs over, the one named last changes fastest.
Arguments:
- hidden_codes: bfloat16 [16, 256, 92160], P('member', None, 'space'), may hold values from -6 to 6
- w_in: bfloat16 [1024, 256], replicated, may hold values from -0.375 to 0.375
- b_in: float32 [1024], replicated, may hold values from -3 to 3
- w_out: bfloat16 [72, 1024], replicated, may hold values from -0.1875 to 0.1875
- b_out: float32 [72], replicated, may hold values from -3 to 3
- target: bfloat16 [72, 92160], P(None, 'space'), may hold values from -6 to 6
- band_start: int32 [32], P('space'), may hold values from 0 to 62, as said below
Outputs:
- code_sensitivity: bfloat16 [16, 256, 92160], P('member', None, 'space')
- grad_w_in: float32 [1024, 256], replicated
- grad_w_out: float32 [72, 1024], replicated
- grad_b_in: float32 [1024], replicated
The draws below stay inside these ranges and needn't reach their ends.
Inputs may be any that keep to these rules, and one draw needn't show every extreme that they name: band_start holds each of 0, 2, 4, ... once, in some order.
All inputs are finite; a program needn't handle non-finite values.
Results may differ from the reference program's by a relative error of at most 0.005.
The reference program's roundings to bfloat16 on the way count: a program that leaves them out, or rounds other values in their place, can miss the bound.
Values may be sent and summed in bfloat16 or wider, within the bound.
A program may use at most 128 MiB of HBM per device.

```python
import math
import jax
import jax.numpy as jnp
from jax import lax

CHANNELS = 72
HID = 1024
LATENT = 256
LON = 1440
ROWS_DEV = 2
MEMBERS = 16
CELLS = 92160
N_SPACE = 32


def draw_band_start(key, part):
    order = jax.random.permutation(jax.random.fold_in(key, 11), N_SPACE)
    return (order * ROWS_DEV).astype(jnp.int32)


def level_of(rng, dims, cuts, smallest, high):
    def one(dim, parts):
        heights = jax.random.uniform(jax.random.fold_in(jax.random.fold_in(rng, 6), dim), (parts,), jnp.float32, smallest / len(cuts), high / len(cuts))
        return jnp.repeat(jnp.exp(heights), dims[dim] // parts).reshape((-1,) + (1,) * (len(dims) - dim - 1))

    level = one(*cuts[0])
    for cut in cuts[1:]:
        level = level * one(*cut)
    return level


def bell_draw(rng, dims, scale, reach, split=(), kind=jnp.bfloat16):
    factor_of = level_of(rng, dims, split, -0.22, 0.18) if split else 1.0
    values = jax.random.normal(rng, dims, jnp.float32) * scale * factor_of
    return jnp.minimum(jnp.maximum(values, -reach), reach).astype(kind)


def setup_inputs(seed: int = 0) -> dict:
    key_list = jax.random.split(jax.random.key(seed), 8)
    hidden_codes = bell_draw(key_list[0], (MEMBERS, LATENT, CELLS), 1.0, 6.0, ((0, 8), (2, 32)))
    w_in = bell_draw(key_list[1], (HID, LATENT), LATENT ** -0.5, 0.375)
    b_in = bell_draw(key_list[2], (HID,), 0.5, 3.0, (), jnp.float32)
    w_out = bell_draw(key_list[3], (CHANNELS, HID), HID ** -0.5, 0.1875)
    b_out = bell_draw(key_list[4], (CHANNELS,), 0.5, 3.0, (), jnp.float32)
    target = bell_draw(key_list[5], (CHANNELS, CELLS), 1.0, 6.0, ((1, 32),))
    band_start = draw_band_start(jax.random.fold_in(key_list[7], 71), 0)
    return dict(hidden_codes=hidden_codes, w_in=w_in, b_in=b_in, w_out=w_out, b_out=b_out, target=target, band_start=band_start)


def slope(diff):
    return diff / jnp.sqrt(diff * diff + 0.0625)

def area_weights(band_start):
    rows = band_start[:, None] + jnp.arange(ROWS_DEV, dtype=jnp.int32)[None, :]
    angle = (rows.astype(jnp.float32) + 0.5) * (math.pi / (ROWS_DEV * N_SPACE)) - math.pi / 2
    return jnp.repeat(jnp.cos(angle).reshape(-1), LON)

def reference(hidden_codes, w_in, b_in, w_out, b_out, target, band_start):
    area = area_weights(band_start)
    members = hidden_codes.shape[0]
    cells = hidden_codes.shape[2]

    def apply_readout(inputs):
        pre = jnp.dot(w_in, inputs, preferred_element_type=jnp.float32) + b_in[:, None]
        act = jax.nn.gelu(pre).astype(jnp.bfloat16)
        return (jnp.dot(w_out, act, preferred_element_type=jnp.float32) + b_out[:, None]).astype(jnp.bfloat16)
    predicted_maps = lax.map(apply_readout, hidden_codes)
    goal = target.astype(jnp.float32)

    def cross_sensitivity(mine):
        diagonal_contribution = mine.astype(jnp.float32)

        def lone_realization(total, other):
            return (total + slope(diagonal_contribution - other.astype(jnp.float32)), None)
        couple_index, discarded_value = lax.scan(lone_realization, jnp.zeros_like(diagonal_contribution), predicted_maps)
        return (area[None, :] * (slope(diagonal_contribution - goal) - couple_index / members)).astype(jnp.bfloat16)
    prediction_sensitivity = lax.map(cross_sensitivity, predicted_maps)

    def reverse_sweep(carry, items):
        inputs, prediction_adjoint = items
        pre = jnp.dot(w_in, inputs, preferred_element_type=jnp.float32) + b_in[:, None]
        act_f, undo = jax.vjp(jax.nn.gelu, pre)
        act = act_f.astype(jnp.bfloat16)
        dact = jnp.dot(w_out.T, prediction_adjoint, preferred_element_type=jnp.float32)
        dpre = undo(dact)[0].astype(jnp.bfloat16)
        dlat = jnp.dot(w_in.T, dpre, preferred_element_type=jnp.float32).astype(jnp.bfloat16)
        adjoint_entry_matrix = carry[0] + jnp.dot(dpre, inputs.T, preferred_element_type=jnp.float32)
        adjoint_exit_matrix = carry[1] + jnp.dot(prediction_adjoint, act.T, preferred_element_type=jnp.float32)
        adjoint_offset = carry[2] + lax.optimization_barrier(jnp.sum(dpre.astype(jnp.float32), axis=1))
        return ((adjoint_entry_matrix, adjoint_exit_matrix, adjoint_offset), dlat)
    opening_offset = (jnp.zeros(w_in.shape, jnp.float32), jnp.zeros(w_out.shape, jnp.float32), jnp.zeros(b_in.shape, jnp.float32))
    (adjoint_entry_matrix, adjoint_exit_matrix, adjoint_offset), code_sensitivity = lax.scan(reverse_sweep, opening_offset, (hidden_codes, prediction_sensitivity))
    scale = 1.0 / math.sqrt(members * (cells // N_SPACE))
    return (code_sensitivity, adjoint_entry_matrix * scale, adjoint_exit_matrix * scale, adjoint_offset * scale)
```

```python
import functools
import math

import jax
import jax.numpy as jnp
from jax import lax
from jax.experimental import pallas as pl
from jax.experimental.pallas import tpu as pltpu
from jax.sharding import PartitionSpec as P

LON = 1440
CHUNK = 384
MESH = pl.DeviceIdType.MESH
K0 = math.sqrt(2.0 / math.pi)
K1 = K0 * 0.044715
F32 = jnp.float32
BF16 = jnp.bfloat16


def kernel(
    geo,
    area_ref, h_ref, w_in_ref, b_in_ref, w_out_ref, b_out_ref, target_ref,
    sens_ref, gin_ref, gout_ref, gb_ref,
    hs, xs, acts, w_in_t, w_out_t, bias, goal, fcast, fpart, ftile, dback,
    acc_in, acc_out, acc_b, gsend, c0, own, p1, c1, z1, c2, fin,
    send_a, recv_a, send_b, recv_b, send_0, recv_0, send_1, recv_1, send_2, recv_2, send_3, recv_3, send_4, recv_4,
):
    n_mem, n_z, cells = geo
    hid, latent = w_in_ref.shape
    chans = w_out_ref.shape[0]
    me = lax.axis_index("member")
    sp = lax.axis_index("space")
    core = lax.rem(sp, 2)
    x_hi = lax.rem(lax.div(sp, 2), 2)
    z = lax.div(sp, 4)
    plane = 2 * n_mem
    my_q = me * 2 + x_hi

    def plane_dev(off):
        q = lax.rem(my_q + off, plane)
        m = lax.div(q, 2)
        s = z * 4 + lax.rem(q, 2) * 2 + core
        return q, {"member": m, "space": s}

    def z_dev(off):
        zz = lax.rem(z + off, n_z)
        return zz, {"space": zz * 4 + x_hi * 2 + core}

    partner = {"space": sp + 1 - 2 * core}

    barrier = pltpu.get_barrier_semaphore()
    for off in range(1, plane):
        pl.semaphore_signal(barrier, inc=1, device_id=plane_dev(off)[1], device_id_type=MESH)
    for off in range(1, n_z):
        pl.semaphore_signal(barrier, inc=1, device_id=z_dev(off)[1], device_id_type=MESH)
    pl.semaphore_signal(barrier, inc=1, device_id=partner, device_id_type=MESH)

    full = cells // CHUNK
    rest = cells - full * CHUNK
    for c in range(n_mem):
        for m in range(2):
            if c < full:
                hs[c, :, m * CHUNK:(m + 1) * CHUNK] = h_ref[m, :, c * CHUNK:(c + 1) * CHUNK]
            else:
                hs[c, :, m * CHUNK:(m + 1) * CHUNK] = jnp.concatenate(
                    [h_ref[m, :, c * CHUNK:cells], jnp.zeros((latent, CHUNK - rest), BF16)], axis=1)
        if c < full:
            goal[c] = target_ref[:, c * CHUNK:(c + 1) * CHUNK].astype(F32)
        else:
            goal[c] = jnp.concatenate(
                [target_ref[:, c * CHUNK:cells].astype(F32), jnp.zeros((chans, CHUNK - rest), F32)], axis=1)
    w_in_t[...] = w_in_ref[...].T
    w_out_t[...] = w_out_ref[...].T
    bias[...] = jnp.broadcast_to(b_in_ref[...], (hid, 128))
    acc_in[...] = jnp.zeros_like(acc_in)
    acc_out[...] = jnp.zeros_like(acc_out)
    acc_b[...] = jnp.zeros_like(acc_b)

    pl.semaphore_wait(barrier, plane - 1 + n_z - 1 + 1)

    def a_copy(d, slot):
        return pltpu.make_async_remote_copy(
            src_ref=fcast.at[d], dst_ref=fpart.at[slot], send_sem=send_a.at[d], recv_sem=recv_a.at[slot],
            device_id={"member": d}, device_id_type=MESH)

    def b_copy(d, slot):
        return pltpu.make_async_remote_copy(
            src_ref=fpart.at[d], dst_ref=dback.at[slot], send_sem=send_b.at[d], recv_sem=recv_b.at[slot],
            device_id={"member": d}, device_id_type=MESH)

    def forward(step, carry):
        c = lax.rem(me + 1 + step, n_mem)
        for j in range(2 * CHUNK // 256):
            cols = slice(j * 256, (j + 1) * 256)
            pre = jnp.dot(w_in_ref[...], hs[c, :, cols], preferred_element_type=F32)
            b2 = bias[...]
            x = pre + jnp.concatenate([b2, b2], axis=1)
            xs[c, :, cols] = x
            t = jnp.tanh(x * (K0 + K1 * (x * x)))
            acts[c, :, cols] = (x * (0.5 * t + 0.5)).astype(BF16)
        out = jnp.dot(w_out_ref[...], acts[c], preferred_element_type=F32) + b_out_ref[...]
        fcast[c] = out.astype(BF16)

        @pl.when(step < n_mem - 1)
        def _():
            a_copy(c, me).start()

        return carry

    lax.fori_loop(0, n_mem, forward, 0)
    fpart[me] = fcast[me]
    for off in range(1, n_mem):
        p = lax.rem(me + n_mem - off, n_mem)
        a_copy(p, p).wait_recv()
    for p in range(n_mem):
        for m in range(2):
            ftile[2 * p + m] = fpart[p, :, m * CHUNK:(m + 1) * CHUNK].astype(F32)

    lanes = lax.broadcasted_iota(jnp.int32, (8, 128), 1)

    def pairs(r, carry):
        rows = pl.ds(pl.multiple_of(r * 8, 8), 8)
        for k in range(CHUNK // 128):
            cols = slice(k * 128, (k + 1) * 128)
            cell = me * CHUNK + k * 128 + lanes
            area = jnp.where(cell < LON, area_ref[0], jnp.where(cell < 2 * LON, area_ref[1], 0.0))
            f = [ftile[i, rows, cols] for i in range(2 * n_mem)]
            total = [None] * (2 * n_mem)
            for i in range(2 * n_mem):
                for j in range(i + 1, 2 * n_mem):
                    d = f[i] - f[j]
                    v = d * lax.rsqrt(d * d + 0.0625)
                    total[i] = v if total[i] is None else total[i] + v
                    total[j] = -v if total[j] is None else total[j] - v
            g = goal[me, rows, cols]
            for i in range(2 * n_mem):
                d = f[i] - g
                v = d * lax.rsqrt(d * d + 0.0625)
                ftile[i, rows, cols] = area * (v - total[i] * (1.0 / (2 * n_mem)))
        return carry

    lax.fori_loop(0, chans // 8, pairs, 0)
    for p in range(n_mem):
        for m in range(2):
            fpart[p, :, m * CHUNK:(m + 1) * CHUNK] = ftile[2 * p + m].astype(BF16)
    for off in range(1, n_mem):
        d = lax.rem(me + off, n_mem)
        b_copy(d, me).start()
    dback[me] = fpart[me]

    def backward(step, carry):
        c = lax.rem(me + n_mem - step, n_mem)

        @pl.when(step > 0)
        def _():
            b_copy(c, c).wait_recv()

        d = dback[c]
        acc_out[:, :chans] += lax.dot_general(
            acts[c], d, (((1,), (1,)), ((), ())), preferred_element_type=F32)
        for j in range(2 * CHUNK // 256):
            cols = slice(j * 256, (j + 1) * 256)
            dact = jnp.dot(w_out_t[...], d[:, cols], preferred_element_type=F32)
            x = xs[c, :, cols]
            x2 = x * x
            t = jnp.tanh(x * (K0 + K1 * x2))
            s = 0.5 * t + 0.5
            slope = s * (1.0 + (x * (1.0 - s)) * (2 * K0 + (6 * K1) * x2))
            dpre = (dact * slope).astype(BF16)
            acts[c, :, cols] = dpre
            wide = dpre.astype(F32)
            acc_b[...] += wide[:, :128] + wide[:, 128:]
        acc_in[...] += lax.dot_general(
            acts[c], hs[c], (((1,), (1,)), ((), ())), preferred_element_type=F32)
        return carry

    lax.fori_loop(0, n_mem, backward, 0)

    def sens_of(c):
        out = jnp.dot(w_in_t[...], acts[c], preferred_element_type=F32).astype(BF16)
        for m in range(2):
            size = CHUNK if c < full else rest
            sens_ref[m, :, c * CHUNK:c * CHUNK + size] = out[:, m * CHUNK:m * CHUNK + size]

    half = hid // 2
    share = half // plane
    lane = lax.broadcasted_iota(jnp.int32, (hid, 128), 1)
    summed_b = jnp.sum(acc_b[...], axis=1, keepdims=True)
    acc_out[...] = jnp.where(lane == chans, summed_b, acc_out[...])
    theirs = pl.ds(pl.multiple_of((1 - core) * half, half), half)
    mine = pl.ds(pl.multiple_of(core * half, half), half)
    gsend[:, :latent] = acc_in[theirs, :].astype(BF16)
    gsend[:, latent:] = acc_out[theirs, :].astype(BF16)
    copy0 = pltpu.make_async_remote_copy(
        src_ref=gsend, dst_ref=c0, send_sem=send_0.at[0], recv_sem=recv_0.at[0], device_id=partner, device_id_type=MESH)
    copy0.start()
    sens_of(0)
    copy0.wait_recv()
    own[:, :latent] = acc_in[mine, :] + c0[:, :latent].astype(F32)
    own[:, latent:] = acc_out[mine, :] + c0[:, latent:].astype(F32)
    for q in range(plane):
        p1[q] = own[q * share:(q + 1) * share, :].astype(BF16)

    def one_copy(q, slot, dev):
        return pltpu.make_async_remote_copy(
            src_ref=p1.at[q], dst_ref=c1.at[slot], send_sem=send_1.at[q], recv_sem=recv_1.at[slot],
            device_id=dev, device_id_type=MESH)

    for off in range(1, plane):
        q, dev = plane_dev(off)
        one_copy(q, my_q, dev).start()
    c1[my_q] = p1[my_q]
    for c in range(1, 4):
        sens_of(c)
    for off in range(1, plane):
        q, dev = plane_dev(plane - off)
        one_copy(q, q, dev).wait_recv()
    part = c1[0].astype(F32)
    for q in range(1, plane):
        part = part + c1[q].astype(F32)
    z1[...] = part.astype(BF16)

    def two_copy(zz, slot, dev):
        return pltpu.make_async_remote_copy(
            src_ref=z1, dst_ref=c2.at[slot], send_sem=send_2.at[zz], recv_sem=recv_2.at[slot],
            device_id=dev, device_id_type=MESH)

    for off in (4, 3, 5, 2, 6, 1, 7):
        zz, dev = z_dev(off)
        two_copy(zz, z, dev).start()
    c2[z] = z1[...]
    for c in range(4, 7):
        sens_of(c)
    for off in range(1, n_z):
        zz, dev = z_dev(off)
        two_copy(zz, zz, dev).wait_recv()
    part = c2[0].astype(F32)
    for zz in range(1, n_z):
        part = part + c2[zz].astype(F32)
    slot = core * plane + my_q
    fin[slot] = part.astype(BF16)

    def three_copy(src_q, dst_q, dev):
        return pltpu.make_async_remote_copy(
            src_ref=fin.at[slot], dst_ref=fin.at[core * plane + src_q], send_sem=send_3.at[dst_q],
            recv_sem=recv_3.at[src_q], device_id=dev, device_id_type=MESH)

    def four_copy(q, c):
        return pltpu.make_async_remote_copy(
            src_ref=fin.at[c * plane + q], dst_ref=fin.at[c * plane + q], send_sem=send_4.at[q],
            recv_sem=recv_4.at[q], device_id=partner, device_id_type=MESH)

    for off in range(1, plane):
        q, dev = plane_dev(off)
        three_copy(my_q, q, dev).start()
    four_copy(my_q, core).start()
    sens_of(7)
    for off in range(1, plane):
        q, dev = plane_dev(plane - off)
        three_copy(q, q, dev).wait_recv()
        four_copy(q, core).start()
    for q in range(plane):
        four_copy(q, 1 - core).wait_recv()

    scale = 1.0 / math.sqrt(2 * n_mem * cells)
    for r in range(2 * plane):
        rows = slice(r * share, (r + 1) * share)
        gin_ref[rows, :] = fin[r, :, :latent].astype(F32) * scale
        acc_out[rows, :] = fin[r, :, latent:].astype(F32) * scale
    flipped = acc_out[...].T
    gout_ref[...] = flipped[:chans, :]
    gb_ref[...] = flipped[chans:chans + 1, :]

    for off in range(1, n_mem):
        d = lax.rem(me + off, n_mem)
        a_copy(d, me).wait_send()
        b_copy(d, me).wait_send()
    copy0.wait_send()
    for off in range(1, plane):
        q, dev = plane_dev(off)
        one_copy(q, my_q, dev).wait_send()
        three_copy(my_q, q, dev).wait_send()
    for off in range(1, n_z):
        zz, dev = z_dev(off)
        two_copy(zz, z, dev).wait_send()
    for q in range(plane):
        four_copy(q, core).wait_send()


def on_device(hidden_codes, w_in, b_in, w_out, b_out, target, band_start):
    mem, latent, cells = hidden_codes.shape
    hid = w_in.shape[0]
    chans = w_out.shape[0]
    rows = cells // LON
    n_mem = lax.axis_size("member")
    n_space = lax.axis_size("space")
    n_z = n_space // 4
    plane = 2 * n_mem
    angle = ((band_start[0] + jnp.arange(rows, dtype=jnp.int32)).astype(F32) + 0.5) * (
        math.pi / (rows * n_space)) - math.pi / 2
    area = jnp.cos(angle)
    wide = latent + 128
    half = hid // 2
    share = half // plane
    vm = pl.BlockSpec(memory_space=pltpu.VMEM)
    dma = pltpu.SemaphoreType.DMA
    sens, gin, gout, gb = pl.pallas_call(
        functools.partial(kernel, (n_mem, n_z, cells)),
        out_shape=(
            jax.ShapeDtypeStruct(hidden_codes.shape, BF16),
            jax.ShapeDtypeStruct((hid, latent), F32),
            jax.ShapeDtypeStruct((chans, hid), F32),
            jax.ShapeDtypeStruct((1, hid), F32),
        ),
        in_specs=[pl.BlockSpec(memory_space=pltpu.SMEM)] + [vm] * 6,
        out_specs=(vm, vm, vm, vm),
        scratch_shapes=[
            pltpu.VMEM((n_mem, latent, 2 * CHUNK), BF16),
            pltpu.VMEM((n_mem, hid, 2 * CHUNK), F32),
            pltpu.VMEM((n_mem, hid, 2 * CHUNK), BF16),
            pltpu.VMEM((latent, hid), BF16),
            pltpu.VMEM((hid, chans), BF16),
            pltpu.VMEM((hid, 128), F32),
            pltpu.VMEM((n_mem, chans, CHUNK), F32),
            pltpu.VMEM((n_mem, chans, 2 * CHUNK), BF16),
            pltpu.VMEM((n_mem, chans, 2 * CHUNK), BF16),
            pltpu.VMEM((2 * n_mem, chans, CHUNK), F32),
            pltpu.VMEM((n_mem, chans, 2 * CHUNK), BF16),
            pltpu.VMEM((hid, latent), F32),
            pltpu.VMEM((hid, 128), F32),
            pltpu.VMEM((hid, 128), F32),
            pltpu.VMEM((half, wide), BF16),
            pltpu.VMEM((half, wide), BF16),
            pltpu.VMEM((half, wide), F32),
            pltpu.VMEM((plane, share, wide), BF16),
            pltpu.VMEM((plane, share, wide), BF16),
            pltpu.VMEM((share, wide), BF16),
            pltpu.VMEM((n_z, share, wide), BF16),
            pltpu.VMEM((2 * plane, share, wide), BF16),
            dma((n_mem,)), dma((n_mem,)), dma((n_mem,)), dma((n_mem,)),
            dma((1,)), dma((1,)), dma((plane,)), dma((plane,)), dma((n_z,)), dma((n_z,)),
            dma((plane,)), dma((plane,)), dma((plane,)), dma((plane,)),
        ],
        compiler_params=pltpu.CompilerParams(
            collective_id=0, has_side_effects=True, vmem_limit_bytes=67043328),
    )(area, hidden_codes, w_in, b_in.reshape(hid, 1), w_out, b_out.reshape(chans, 1), target)
    return sens, gin, gout, gb.reshape(hid)


def solution(mesh):
    in_specs = (P("member", None, "space"), P(), P(), P(), P(), P(None, "space"), P("space"))
    out_specs = (P("member", None, "space"), P(), P(), P())
    return jax.shard_map(
        on_device, mesh=mesh, in_specs=in_specs, out_specs=out_specs, check_vma=False
    )
```

```python
import functools
import math

import jax
import jax.numpy as jnp
from jax import lax
from jax.experimental import pallas as pl
from jax.experimental.pallas import tpu as pltpu
from jax.sharding import PartitionSpec as P

LON = 1440
SUBS = (256, 128)
CHUNK = sum(SUBS)
PARTS = 2
LATE = 2
MESH = pl.DeviceIdType.MESH
K0 = math.sqrt(2.0 / math.pi)
K1 = K0 * 0.044715
F32 = jnp.float32
BF16 = jnp.bfloat16


class Mark:
    def __init__(self):
        self.cm = None

    def __call__(self, name):
        if self.cm is not None:
            self.cm.__exit__(None, None, None)
            self.cm = None
        if name:
            self.cm = jax.named_scope(name)
            self.cm.__enter__()


def kernel(
    geo,
    area_ref, h_ref, w_in_hbm, b_in_hbm, w_out_hbm, b_out_hbm, target_hbm,
    sens_ref, fin_ref,
    w_in_ref, b_in_ref, w_out_ref, b_out_ref, target_ref,
    hs0, hs1, slopes0, slopes1, acts0, acts1, fcast0, fcast1, fpart0, fpart1, dback0, dback1,
    w_half, w_in_t, w_out_t, bias, bias_out, goal, ftile,
    acc_in, acc_out, acc_b, gsend, c0, own, p1, c1, z1, c2, fin,
    send_a, recv_a, send_b, recv_b, send_0, recv_0, send_1, recv_1, send_2, recv_2, send_3, recv_3, send_4, recv_4,
    load, store, keep, given,
):
    n_mem, n_z, cells = geo
    hid, latent = w_in_hbm.shape
    chans = w_out_hbm.shape[0]
    hs, slopes, acts = (hs0, hs1), (slopes0, slopes1), (acts0, acts1)
    fcast, fpart, dback = (fcast0, fcast1), (fpart0, fpart1), (dback0, dback1)
    me = lax.axis_index("member")
    sp = lax.axis_index("space")
    core = lax.rem(sp, 2)
    x_hi = lax.rem(lax.div(sp, 2), 2)
    z = lax.div(sp, 4)
    plane = 2 * n_mem
    my_q = me * 2 + x_hi
    full = cells // CHUNK
    rest = cells - full * CHUNK
    first_at = (0, SUBS[0])

    def plane_dev(off):
        q = lax.rem(my_q + off, plane)
        return q, {"member": lax.div(q, 2), "space": z * 4 + lax.rem(q, 2) * 2 + core}

    def z_dev(off):
        zz = lax.rem(z + off, n_z)
        return zz, {"space": zz * 4 + x_hi * 2 + core}

    partner = {"space": sp + 1 - 2 * core}
    mark = Mark()
    mark('entry')

    weights = [
        pltpu.make_async_copy(far, near, given.at[i]) for i, (far, near) in enumerate((
            (w_in_hbm, w_in_ref), (w_out_hbm, w_out_ref), (b_in_hbm, b_in_ref), (b_out_hbm, b_out_ref),
            (target_hbm, target_ref)))]
    for copy in weights:
        copy.start()

    def pieces(c, b, size):
        return [(m, pl.ds(c * CHUNK + first_at[b], size), pl.ds(m * SUBS[b], size)) for m in range(2)]

    def load_copies(c, b, size):
        return [
            pltpu.make_async_copy(h_ref.at[m, far, :], hs[b].at[c, near, :], load.at[b * n_mem + c])
            for m, far, near in pieces(c, b, size)]

    def store_copies(c, b, size):
        return [
            pltpu.make_async_copy(hs[b].at[c, near, :], sens_ref.at[m, far, :], store.at[0])
            for m, far, near in pieces(c, b, size)]

    def load_wait(c, b, size):
        pltpu.make_async_copy(
            h_ref.at[0, pl.ds(0, 2 * size), :], hs[b].at[c, pl.ds(0, 2 * size), :], load.at[b * n_mem + c]).wait()

    all_pieces = [(c, 0, SUBS[0] if c < full else rest) for c in range(n_mem)] + [(c, 1, SUBS[1]) for c in range(full)]
    for piece in all_pieces:
        for copy in load_copies(*piece):
            copy.start()

    barrier = pltpu.get_barrier_semaphore()
    for off in range(1, plane):
        pl.semaphore_signal(barrier, inc=1, device_id=plane_dev(off)[1], device_id_type=MESH)
    for off in range(1, n_z):
        pl.semaphore_signal(barrier, inc=1, device_id=z_dev(off)[1], device_id_type=MESH)
    pl.semaphore_signal(barrier, inc=1, device_id=partner, device_id_type=MESH)

    mark('prep')
    for copy in weights:
        copy.wait()
    for m in range(2):
        hs0[full, m * SUBS[0] + rest:(m + 1) * SUBS[0], :] = jnp.zeros((SUBS[0] - rest, latent), BF16)
    for c in range(n_mem):
        if c < full:
            goal[c] = target_ref[:, c * CHUNK:(c + 1) * CHUNK].astype(F32)
        else:
            goal[c] = jnp.concatenate(
                [target_ref[:, c * CHUNK:cells].astype(F32), jnp.zeros((chans, CHUNK - rest), F32)], axis=1)
    w_in_t[...] = w_in_ref[...].T
    w_half[...] = w_in_ref[...] * 0.5
    w_out_t[...] = w_out_ref[...].T * 0.5
    bias[...] = jnp.broadcast_to(0.5 * b_in_ref[...], (128, hid)).T
    bias_out[...] = jnp.broadcast_to(b_out_ref[...], (128, chans)).T
    acc_in[...] = jnp.zeros_like(acc_in)
    acc_out[...] = jnp.zeros_like(acc_out)
    acc_b[...] = jnp.zeros_like(acc_b)

    def a_copy(b, d, slot):
        return pltpu.make_async_remote_copy(
            src_ref=fcast[b].at[d], dst_ref=fpart[b].at[slot], send_sem=send_a.at[b],
            recv_sem=recv_a.at[b], device_id={"member": d}, device_id_type=MESH)

    def b_copy(b, d, slot):
        return pltpu.make_async_remote_copy(
            src_ref=fpart[b].at[d], dst_ref=dback[b].at[slot], send_sem=send_b.at[b],
            recv_sem=recv_b.at[b * n_mem + slot], device_id={"member": d}, device_id_type=MESH)

    def took(ref, sem):
        pltpu.make_async_copy(ref, ref, sem).wait()

    def forward_chunk(b, c):
        b2 = jnp.concatenate([bias[...]] * 2, axis=1)
        bo2 = jnp.concatenate([bias_out[...]] * 2, axis=1)
        for j in range(2 * SUBS[b] // 256):
            cols = slice(j * 256, (j + 1) * 256)
            x = lax.dot_general(
                w_half[...], hs[b][c, cols, :], (((1,), (1,)), ((), ())), preferred_element_type=F32) + b2
            poly = 2.0 * K0 + (8.0 * K1) * (x * x)
            t = jnp.tanh(x * poly)
            p = 1.0 + t
            a = x * p
            slopes[b][c, :, cols] = p + (a * (1.0 - t)) * (3.0 * poly - 4.0 * K0)
            a = a.astype(BF16)
            acts[b][c, :, cols] = a
            fcast[b][c, :, cols] = (jnp.dot(w_out_ref[...], a, preferred_element_type=F32) + bo2).astype(BF16)

    mark('forward0')

    def forward0(step, carry):
        c = lax.rem(me + 1 + step, n_mem)

        @pl.when(c < full)
        def _():
            load_wait(c, 0, SUBS[0])

        @pl.when(c == full)
        def _():
            load_wait(c, 0, rest)

        forward_chunk(0, c)

        @pl.when(step == LATE)
        def _():
            pl.semaphore_wait(barrier, plane - 1 + n_z - 1 + 1)
            for early in range(LATE):
                a_copy(0, lax.rem(me + 1 + early, n_mem), me).start()

        @pl.when((step >= LATE) & (step < n_mem - 1))
        def _():
            a_copy(0, c, me).start()

        return carry

    lax.fori_loop(0, n_mem, forward0, 0)
    mark('forward1')

    def forward1(step, carry):
        c = lax.rem(me + 1 + step, n_mem)

        @pl.when(c < full)
        def _():
            load_wait(c, 1, SUBS[1])
            forward_chunk(1, c)

            @pl.when(step < n_mem - 1)
            def _():
                a_copy(1, c, me).start()

        return carry

    lax.fori_loop(0, n_mem, forward1, 0)

    lanes = lax.broadcasted_iota(jnp.int32, (8, 128), 1)

    def meet(b):
        size = SUBS[b]
        at = first_at[b]
        fpart[b][me] = fcast[b][me]
        took(fpart[b].at[pl.ds(0, n_mem - 1)], recv_a.at[b])
        mark(f'pairs{b}')
        for p in range(n_mem):
            for m in range(2):
                ftile[2 * p + m, :, at:at + size] = fpart[b][p, :, m * size:(m + 1) * size].astype(F32)

        def pairs(r, carry):
            rows = pl.ds(pl.multiple_of(r * 8, 8), 8)
            for k in range(size // 128):
                cols = slice(at + k * 128, at + (k + 1) * 128)
                cell = me * CHUNK + (at + k * 128) + lanes
                area = jnp.where(cell < LON, area_ref[0], jnp.where(cell < 2 * LON, area_ref[1], 0.0))
                f = [ftile[i, rows, cols] for i in range(2 * n_mem)]
                total = [None] * (2 * n_mem)
                for i in range(2 * n_mem):
                    for j in range(i + 1, 2 * n_mem):
                        d = f[i] - f[j]
                        v = d * lax.rsqrt(d * d + 0.0625)
                        total[i] = v if total[i] is None else total[i] + v
                        total[j] = -v if total[j] is None else total[j] - v
                g = goal[me, rows, cols]
                for i in range(2 * n_mem):
                    d = f[i] - g
                    v = d * lax.rsqrt(d * d + 0.0625)
                    ftile[i, rows, cols] = area * (v - total[i] * (1.0 / (2 * n_mem)))
            return carry

        lax.fori_loop(0, chans // 8, pairs, 0)
        for p in range(n_mem):
            for m in range(2):
                fpart[b][p, :, m * size:(m + 1) * size] = ftile[2 * p + m, :, at:at + size].astype(BF16)
        for off in range(1, n_mem):
            d = lax.rem(me + off, n_mem)
            b_copy(b, d, me).start()
        dback[b][me] = fpart[b][me]

    mark('waitA0')
    meet(0)
    mark('waitA1')

    @pl.when(me < full)
    def _():
        meet(1)

    def backward_chunk(b, c):
        d = dback[b][c]
        acc_out[:, :chans] += lax.dot_general(
            acts[b][c], d, (((1,), (1,)), ((), ())), preferred_element_type=F32)
        for j in range(2 * SUBS[b] // 256):
            cols = slice(j * 256, (j + 1) * 256)
            dact = jnp.dot(w_out_t[...], d[:, cols], preferred_element_type=F32)
            dpre = (dact * slopes[b][c, :, cols]).astype(BF16)
            acts[b][c, :, cols] = dpre
            wide = dpre.astype(F32)
            acc_b[...] += wide[:, :128] + wide[:, 128:]
        acc_in[...] += jnp.dot(acts[b][c], hs[b][c], preferred_element_type=F32)

    def backward0(step, carry):
        c = lax.rem(me + n_mem - step, n_mem)

        @pl.when(step > 0)
        def _():
            b_copy(0, c, c).wait_recv()

        backward_chunk(0, c)
        return carry

    def backward1(step, carry):
        c = lax.rem(me + n_mem - step, n_mem)

        @pl.when(c < full)
        def _():
            @pl.when(step > 0)
            def _():
                b_copy(1, c, c).wait_recv()

            backward_chunk(1, c)

        return carry

    mark('backward0')
    lax.fori_loop(0, n_mem, backward0, 0)
    mark('backward1')
    lax.fori_loop(0, n_mem, backward1, 0)

    def sens_of(*chunks):
        for c in chunks:
            for piece in all_pieces:
                if piece[0] == c:
                    b = piece[1]
                    hs[b][c] = jnp.dot(w_in_t[...], acts[b][c], preferred_element_type=F32).T.astype(BF16)
                    for copy in store_copies(*piece):
                        copy.start()

    mark('gradprep')
    half = hid // 2
    block = half // PARTS
    share = block // plane
    lane = lax.broadcasted_iota(jnp.int32, (hid, 128), 1)
    summed_b = jnp.sum(acc_b[...], axis=1, keepdims=True)
    acc_out[...] = jnp.where(lane == chans, summed_b, acc_out[...])

    def zero_copy(r):
        return pltpu.make_async_remote_copy(
            src_ref=gsend.at[r], dst_ref=c0.at[r], send_sem=send_0.at[r], recv_sem=recv_0.at[r],
            device_id=partner, device_id_type=MESH)

    def one_copy(r, q, slot, dev):
        return pltpu.make_async_remote_copy(
            src_ref=p1.at[r, q], dst_ref=c1.at[r, slot], send_sem=send_1.at[r],
            recv_sem=recv_1.at[r], device_id=dev, device_id_type=MESH)

    def two_copy(r, zz, slot, dev):
        return pltpu.make_async_remote_copy(
            src_ref=z1.at[r], dst_ref=c2.at[r, slot], send_sem=send_2.at[r],
            recv_sem=recv_2.at[r], device_id=dev, device_id_type=MESH)

    def at_fin(r, k, q):
        return (k * PARTS + r) * plane + q

    def three_copy(r, src_q, dst_q, dev):
        return pltpu.make_async_remote_copy(
            src_ref=fin.at[at_fin(r, core, my_q)], dst_ref=fin.at[at_fin(r, core, src_q)],
            send_sem=send_3.at[r], recv_sem=recv_3.at[r],
            device_id=dev, device_id_type=MESH)

    def of_core(r, k):
        return pl.ds(at_fin(r, k, 0), plane)

    def four_copy(r):
        mine = fin.at[of_core(r, core)]
        return pltpu.make_async_remote_copy(
            src_ref=mine, dst_ref=mine, send_sem=send_4.at[r], recv_sem=recv_4.at[r],
            device_id=partner, device_id_type=MESH)

    def fin_out(r, k):
        return pltpu.make_async_copy(fin.at[of_core(r, k)], fin_ref.at[of_core(r, k)], keep.at[0])

    for r in range(PARTS):
        theirs = pl.ds(pl.multiple_of((1 - core) * half + r * block, block), block)
        gsend[r, :, :latent] = acc_in[theirs, :].astype(BF16)
        gsend[r, :, latent:] = acc_out[theirs, :].astype(BF16)
        zero_copy(r).start()
    mark('sens0')
    sens_of(0)
    for r in range(PARTS):
        mark(f'wait0.{r}')
        zero_copy(r).wait_recv()
        mark(f'sum0.{r}')
        mine = pl.ds(pl.multiple_of(core * half + r * block, block), block)
        own[:, :latent] = acc_in[mine, :] + c0[r, :, :latent].astype(F32)
        own[:, latent:] = acc_out[mine, :] + c0[r, :, latent:].astype(F32)
        for q in range(plane):
            p1[r, q] = own[q * share:(q + 1) * share, :].astype(BF16)
        for off in range(1, plane):
            q, dev = plane_dev(off)
            one_copy(r, q, my_q, dev).start()
        c1[r, my_q] = p1[r, my_q]
    mark('sens1')
    sens_of(1, 2, 3)
    for r in range(PARTS):
        mark(f'wait1.{r}')
        took(c1.at[r, pl.ds(0, plane - 1)], recv_1.at[r])
        mark(f'sum1.{r}')
        part = c1[r, 0].astype(F32)
        for q in range(1, plane):
            part = part + c1[r, q].astype(F32)
        z1[r] = part.astype(BF16)
        for off in (4, 3, 5, 2, 6, 1, 7):
            zz, dev = z_dev(off)
            two_copy(r, zz, z, dev).start()
        c2[r, z] = z1[r]
        mark(f'sens2.{r}')
        if r == 0:
            sens_of(4, 5)
        if r == PARTS - 1:
            sens_of(6)
    for r in range(PARTS):
        mark(f'wait2.{r}')
        took(c2.at[r, pl.ds(0, n_z - 1)], recv_2.at[r])
        mark(f'sum2.{r}')
        part = c2[r, 0].astype(F32)
        for zz in range(1, n_z):
            part = part + c2[r, zz].astype(F32)
        fin[at_fin(r, core, my_q)] = part.astype(BF16)
        for off in range(1, plane):
            q, dev = plane_dev(off)
            three_copy(r, my_q, q, dev).start()
        if r == 0:
            sens_of(7)
    for r in range(PARTS):
        mark(f'wait3.{r}')
        took(fin.at[pl.ds(0, plane - 1)], recv_3.at[r])
        four_copy(r).start()
        fin_out(r, core).start()
    for r in range(PARTS):
        mark(f'wait4.{r}')
        took(fin.at[pl.ds(0, plane)], recv_4.at[r])
        fin_out(r, 1 - core).start()
    mark('drain')
    took(sens_ref, store.at[0])
    took(fcast[0].at[pl.ds(0, n_mem - 1)], send_a.at[0])
    took(fpart[0].at[pl.ds(0, n_mem - 1)], send_b.at[0])

    @pl.when(me < full)
    def _():
        took(fcast[1].at[pl.ds(0, full - 1)], send_a.at[1])
        took(fpart[1].at[pl.ds(0, n_mem - 1)], send_b.at[1])

    @pl.when(me == full)
    def _():
        took(fcast[1].at[pl.ds(0, full)], send_a.at[1])

    for r in range(PARTS):
        zero_copy(r).wait_send()
        took(c1.at[r, pl.ds(0, plane - 1)], send_1.at[r])
        took(c2.at[r, pl.ds(0, n_z - 1)], send_2.at[r])
        took(fin.at[pl.ds(0, plane - 1)], send_3.at[r])
        took(fin.at[pl.ds(0, plane)], send_4.at[r])
    took(fin_ref, keep.at[0])
    mark(None)


def finish(geo, sens_ref, fin_ref, out_ref, gin_ref, gout_ref, gb_ref, held, fin, gin, gout, gb, come, go):
    scale, latent, chans = geo
    n = held.shape[0]
    rows = held.shape[2]
    mem = held.shape[1]

    def come_in(i, m):
        return pltpu.make_async_copy(sens_ref.at[m, pl.ds(i * rows, rows), :], held.at[i, m], come.at[mem * i + m])

    def go_out(i, m):
        return pltpu.make_async_copy(held.at[i, m], out_ref.at[m, pl.ds(i * rows, rows), :], go.at[mem * i + m])

    fin_in = pltpu.make_async_copy(fin_ref, fin, come.at[mem * n])
    gin_out = pltpu.make_async_copy(gin, gin_ref, go.at[mem * n])
    gout_out = pltpu.make_async_copy(gout, gout_ref, go.at[mem * n + 1])
    gb_out = pltpu.make_async_copy(gb, gb_ref, go.at[mem * n + 2])
    fin_in.start()
    both = [(i, m) for i in range(n) for m in range(mem)]
    for i, m in both:
        come_in(i, m).start()
    fin_in.wait()
    share = fin.shape[1]
    for r in range(fin.shape[0]):
        gin[r * share:(r + 1) * share, :] = fin[r, :, :latent].astype(F32) * scale
    gin_out.start()
    flipped = fin[:, :, latent:].astype(F32).reshape(gin.shape[0], -1).T * scale
    gout[...] = flipped[:chans, :]
    gb[...] = flipped[chans:chans + 1, :]
    gout_out.start()
    gb_out.start()
    for i, m in both:
        come_in(i, m).wait()
        go_out(i, m).start()
    for i, m in both:
        go_out(i, m).wait()
    gin_out.wait()
    gout_out.wait()
    gb_out.wait()


def on_device(hidden_codes, w_in, b_in, w_out, b_out, target, band_start):
    mem, latent, cells = hidden_codes.shape
    hid = w_in.shape[0]
    chans = w_out.shape[0]
    rows = cells // LON
    n_mem = lax.axis_size("member")
    n_space = lax.axis_size("space")
    n_z = n_space // 4
    plane = 2 * n_mem
    angle = ((band_start[0] + jnp.arange(rows, dtype=jnp.int32)).astype(F32) + 0.5) * (
        math.pi / (rows * n_space)) - math.pi / 2
    area = jnp.cos(angle)
    wide = latent + 128
    half = hid // 2
    block = half // PARTS
    share = block // plane
    vm = pl.BlockSpec(memory_space=pltpu.VMEM)
    hbm = pl.BlockSpec(memory_space=pl.ANY)
    dma = pltpu.SemaphoreType.DMA

    def by_sub(make):
        return [make(2 * size) for size in SUBS]

    sens, fin = pl.pallas_call(
        functools.partial(kernel, (n_mem, n_z, cells)),
        out_shape=(
            jax.ShapeDtypeStruct((mem, cells, latent), BF16),
            jax.ShapeDtypeStruct((2 * PARTS * plane, share, wide), BF16),
        ),
        in_specs=[pl.BlockSpec(memory_space=pltpu.SMEM)] + [hbm] * 6,
        out_specs=(hbm, hbm),
        scratch_shapes=[
            pltpu.VMEM((hid, latent), BF16),
            pltpu.VMEM((1, hid), F32),
            pltpu.VMEM((chans, hid), BF16),
            pltpu.VMEM((1, chans), F32),
            pltpu.VMEM((chans, cells), BF16),
            *by_sub(lambda n: pltpu.VMEM((n_mem, n, latent), BF16)),
            *by_sub(lambda n: pltpu.VMEM((n_mem, hid, n), F32)),
            *by_sub(lambda n: pltpu.VMEM((n_mem, hid, n), BF16)),
            *by_sub(lambda n: pltpu.VMEM((n_mem, chans, n), BF16)),
            *by_sub(lambda n: pltpu.VMEM((n_mem, chans, n), BF16)),
            *by_sub(lambda n: pltpu.VMEM((n_mem, chans, n), BF16)),
            pltpu.VMEM((hid, latent), BF16),
            pltpu.VMEM((latent, hid), BF16),
            pltpu.VMEM((hid, chans), BF16),
            pltpu.VMEM((hid, 128), F32),
            pltpu.VMEM((chans, 128), F32),
            pltpu.VMEM((n_mem, chans, CHUNK), F32),
            pltpu.VMEM((2 * n_mem, chans, CHUNK), F32),
            pltpu.VMEM((hid, latent), F32),
            pltpu.VMEM((hid, 128), F32),
            pltpu.VMEM((hid, 128), F32),
            pltpu.VMEM((PARTS, block, wide), BF16),
            pltpu.VMEM((PARTS, block, wide), BF16),
            pltpu.VMEM((block, wide), F32),
            pltpu.VMEM((PARTS, plane, share, wide), BF16),
            pltpu.VMEM((PARTS, plane, share, wide), BF16),
            pltpu.VMEM((PARTS, share, wide), BF16),
            pltpu.VMEM((PARTS, n_z, share, wide), BF16),
            pltpu.VMEM((2 * PARTS * plane, share, wide), BF16),
            dma((2,)), dma((2,)), dma((2,)), dma((2 * n_mem,)),
            *[dma((PARTS,))] * 10,
            dma((2 * n_mem,)), dma((1,)), dma((1,)), dma((5,)),
        ],
        compiler_params=pltpu.CompilerParams(
            collective_id=0, has_side_effects=True, vmem_limit_bytes=67043328),
    )(area, jnp.swapaxes(hidden_codes, 1, 2), w_in, b_in.reshape(1, hid), w_out, b_out.reshape(1, chans), target)
    pieces = 6
    sens, gin, gout, gb = pl.pallas_call(
        functools.partial(finish, (1.0 / math.sqrt(2 * n_mem * cells), latent, chans)),
        out_shape=(
            jax.ShapeDtypeStruct((mem, cells, latent), BF16),
            jax.ShapeDtypeStruct((hid, latent), F32),
            jax.ShapeDtypeStruct((chans, hid), F32),
            jax.ShapeDtypeStruct((1, hid), F32),
        ),
        in_specs=[hbm, hbm],
        out_specs=(hbm, hbm, hbm, hbm),
        scratch_shapes=[
            pltpu.VMEM((pieces, mem, cells // pieces, latent), BF16),
            pltpu.VMEM((2 * PARTS * plane, share, wide), BF16),
            pltpu.VMEM((hid, latent), F32),
            pltpu.VMEM((chans, hid), F32),
            pltpu.VMEM((1, hid), F32),
            dma((pieces * mem + 1,)), dma((pieces * mem + 3,)),
        ],
    )(sens, fin)
    return jnp.swapaxes(sens, 1, 2), gin, gout, gb.reshape(hid)


def solution(mesh):
    in_specs = (P("member", None, "space"), P(), P(), P(), P(), P(None, "space"), P("space"))
    out_specs = (P("member", None, "space"), P(), P(), P())
    return jax.shard_map(
        on_device, mesh=mesh, in_specs=in_specs, out_specs=out_specs, check_vma=False
    )
```

```python
import functools
import math

import jax
import jax.numpy as jnp
from jax import lax
from jax.experimental import pallas as pl
from jax.experimental.pallas import tpu as pltpu
from jax.sharding import PartitionSpec as P

LON = 1440
SUBS = (256, 128)
CHUNK = sum(SUBS)
PARTS = 4
LATE = 3
CUT_F = 8
CUT_B = 1
MESH = pl.DeviceIdType.MESH
K0 = math.sqrt(2.0 / math.pi)
K1 = K0 * 0.044715
F32 = jnp.float32
BF16 = jnp.bfloat16


class Mark:
    def __init__(self):
        self.cm = None

    def __call__(self, name):
        if self.cm is not None:
            self.cm.__exit__(None, None, None)
            self.cm = None
        if name:
            self.cm = jax.named_scope(name)
            self.cm.__enter__()


def kernel(
    geo,
    band_ref, h_ref, w_in_ref, b_in_ref, w_out_ref, b_out_ref, target_ref,
    sens_ref, fin_ref,
    hs0, hs1, slopes0, slopes1, acts0, acts1, fcast0, fcast1, fpart0, fpart1, dback0, dback1,
    areas, w_half, w_in_t, w_out_t, bias, bias_out, goal, ftile,
    acc_in, acc_out, acc_b, gsend, c0, own, p1, c1, z1, c2, fin,
    send_a, recv_a, send_b, recv_b, send_0, recv_0, send_1, recv_1, send_2, recv_2, send_3, recv_3, send_4, recv_4,
    load, store, keep,
):
    n_mem, n_z, cells, lat_rows = geo
    hid, latent = w_in_ref.shape
    chans = w_out_ref.shape[0]
    hs, slopes, acts = (hs0, hs1), (slopes0, slopes1), (acts0, acts1)
    fcast, fpart, dback = (fcast0, fcast1), (fpart0, fpart1), (dback0, dback1)
    me = lax.axis_index("member")
    sp = lax.axis_index("space")
    core = lax.rem(sp, 2)
    x_hi = lax.rem(lax.div(sp, 2), 2)
    z = lax.div(sp, 4)
    plane = 2 * n_mem
    my_q = me * 2 + x_hi
    full = cells // CHUNK
    rest = cells - full * CHUNK
    first_at = (0, SUBS[0])

    def plane_dev(off):
        q = lax.rem(my_q + off, plane)
        return q, {"member": lax.div(q, 2), "space": z * 4 + lax.rem(q, 2) * 2 + core}

    def z_dev(off):
        zz = lax.rem(z + off, n_z)
        return zz, {"space": zz * 4 + x_hi * 2 + core}

    partner = {"space": sp + 1 - 2 * core}
    mark = Mark()
    mark('entry')

    def pieces(c, b, size):
        return [(m, pl.ds(c * CHUNK + first_at[b], size), pl.ds(m * SUBS[b], size)) for m in range(2)]

    def load_copies(c, b, size):
        return [
            pltpu.make_async_copy(h_ref.at[m, far, :], hs[b].at[c, near, :], load.at[b * n_mem + c])
            for m, far, near in pieces(c, b, size)]

    def store_copies(c, b, size):
        return [
            pltpu.make_async_copy(hs[b].at[c, near, :], sens_ref.at[m, far, :], store.at[0])
            for m, far, near in pieces(c, b, size)]

    def load_wait(c, b, size):
        pltpu.make_async_copy(
            h_ref.at[0, pl.ds(0, 2 * size), :], hs[b].at[c, pl.ds(0, 2 * size), :], load.at[b * n_mem + c]).wait()

    all_pieces = [(c, 0, SUBS[0] if c < full else rest) for c in range(n_mem)] + [(c, 1, SUBS[1]) for c in range(full)]
    for piece in all_pieces:
        for copy in load_copies(*piece):
            copy.start()

    barrier = pltpu.get_barrier_semaphore()
    for off in range(1, plane):
        pl.semaphore_signal(barrier, inc=1, device_id=plane_dev(off)[1], device_id_type=MESH)
    for off in range(1, n_z):
        pl.semaphore_signal(barrier, inc=1, device_id=z_dev(off)[1], device_id_type=MESH)
    pl.semaphore_signal(barrier, inc=1, device_id=partner, device_id_type=MESH)

    mark('prep')
    for m in range(2):
        hs0[full, m * SUBS[0] + rest:(m + 1) * SUBS[0], :] = jnp.zeros((SUBS[0] - rest, latent), BF16)
    for c in range(n_mem):
        if c < full:
            goal[c] = target_ref[:, c * CHUNK:(c + 1) * CHUNK].astype(F32)
        else:
            goal[c] = jnp.concatenate(
                [target_ref[:, c * CHUNK:cells].astype(F32), jnp.zeros((chans, CHUNK - rest), F32)], axis=1)
    w_in_t[...] = w_in_ref[...].T
    cell = me * CHUNK + lax.broadcasted_iota(jnp.int32, (8, CHUNK), 1)
    row = band_ref[0] + jnp.where(cell < LON, 0, 1)
    angle = (row.astype(F32) + 0.5) * (math.pi / lat_rows) - math.pi / 2
    areas[...] = jnp.where(cell < cells, jnp.cos(angle), 0.0)
    w_half[...] = w_in_ref[...] * 0.5
    w_out_t[...] = w_out_ref[...].T * 0.5
    bias[...] = jnp.broadcast_to(0.5 * b_in_ref[...], (128, hid)).T
    bias_out[...] = jnp.broadcast_to(b_out_ref[...], (128, chans)).T
    acc_in[...] = jnp.zeros_like(acc_in)
    acc_out[...] = jnp.zeros_like(acc_out)
    acc_b[...] = jnp.zeros_like(acc_b)

    def a_copy(b, d, slot):
        return pltpu.make_async_remote_copy(
            src_ref=fcast[b].at[d], dst_ref=fpart[b].at[slot], send_sem=send_a.at[b],
            recv_sem=recv_a.at[b], device_id={"member": d}, device_id_type=MESH)

    def b_copy(b, d, slot):
        return pltpu.make_async_remote_copy(
            src_ref=fpart[b].at[d], dst_ref=dback[b].at[slot], send_sem=send_b.at[b],
            recv_sem=recv_b.at[b * n_mem + slot], device_id={"member": d}, device_id_type=MESH)

    def took(ref, sem):
        pltpu.make_async_copy(ref, ref, sem).wait()

    def forward_chunk(b, c):
        b2 = jnp.concatenate([bias[...]] * 2, axis=1)
        bo2 = jnp.concatenate([bias_out[...]] * 2, axis=1)
        for j in range(2 * SUBS[b] // 256):
            cols = slice(j * 256, (j + 1) * 256)
            x = lax.dot_general(
                w_half[...], hs[b][c, cols, :], (((1,), (1,)), ((), ())), preferred_element_type=F32) + b2
            poly = 2.0 * K0 + (8.0 * K1) * (x * x)
            t = jnp.tanh(x * poly)
            p = 1.0 + t
            a = x * p
            slopes[b][c, :, cols] = p + (a * (1.0 - t)) * (3.0 * poly - 4.0 * K0)
            a = a.astype(BF16)
            acts[b][c, :, cols] = a
            fcast[b][c, :, cols] = (jnp.dot(w_out_ref[...], a, preferred_element_type=F32) + bo2).astype(BF16)

    mark('forward0')

    def forward0(step, carry):
        c = lax.rem(me + 1 + step, n_mem)

        @pl.when(c < full)
        def _():
            load_wait(c, 0, SUBS[0])

        @pl.when(c == full)
        def _():
            load_wait(c, 0, rest)

        forward_chunk(0, c)

        @pl.when(step == LATE)
        def _():
            pl.semaphore_wait(barrier, plane - 1 + n_z - 1 + 1)
            for early in range(LATE):
                a_copy(0, lax.rem(me + 1 + early, n_mem), me).start()

        @pl.when((step >= LATE) & (step < n_mem - 1))
        def _():
            a_copy(0, c, me).start()

        return carry

    lax.fori_loop(0, n_mem, forward0, 0)
    mark('forward1')

    def forward1(step, carry):
        c = lax.rem(me + 1 + step, n_mem)

        @pl.when(c < full)
        def _():
            load_wait(c, 1, SUBS[1])
            forward_chunk(1, c)

            @pl.when(step < n_mem - 1)
            def _():
                a_copy(1, c, me).start()

        return carry


    def meet(b):
        size = SUBS[b]
        at = first_at[b]
        fpart[b][me] = fcast[b][me]
        took(fpart[b].at[pl.ds(0, n_mem - 1)], recv_a.at[b])
        if b == 0:
            mark('pairs0')
        for p in range(n_mem):
            for m in range(2):
                ftile[2 * p + m, :, at:at + size] = fpart[b][p, :, m * size:(m + 1) * size].astype(F32)

        def pairs(r, carry):
            rows = pl.ds(pl.multiple_of(r * 8, 8), 8)
            for k in range(size // 128):
                cols = slice(at + k * 128, at + (k + 1) * 128)
                area = areas[:, cols]
                f = [ftile[i, rows, cols] for i in range(2 * n_mem)]
                total = [None] * (2 * n_mem)
                for i in range(2 * n_mem):
                    for j in range(i + 1, 2 * n_mem):
                        d = f[i] - f[j]
                        v = d * lax.rsqrt(d * d + 0.0625)
                        total[i] = v if total[i] is None else total[i] + v
                        total[j] = -v if total[j] is None else total[j] - v
                g = goal[me, rows, cols]
                for i in range(2 * n_mem):
                    d = f[i] - g
                    v = d * lax.rsqrt(d * d + 0.0625)
                    ftile[i, rows, cols] = area * (v - total[i] * (1.0 / (2 * n_mem)))
            return carry

        lax.fori_loop(0, chans // 8, pairs, 0)
        for p in range(n_mem):
            for m in range(2):
                fpart[b][p, :, m * size:(m + 1) * size] = ftile[2 * p + m, :, at:at + size].astype(BF16)
        for off in range(1, n_mem):
            d = lax.rem(me + off, n_mem)
            b_copy(b, d, me).start()
        dback[b][me] = fpart[b][me]

    def backward_chunk(b, *chunks):
        acc_out[:, :chans] += sum(
            lax.dot_general(acts[b][c], dback[b][c], (((1,), (1,)), ((), ())), preferred_element_type=F32)
            for c in chunks)
        for c in chunks:
            for j in range(2 * SUBS[b] // 256):
                cols = slice(j * 256, (j + 1) * 256)
                dact = jnp.dot(w_out_t[...], dback[b][c, :, cols], preferred_element_type=F32)
                dpre = (dact * slopes[b][c, :, cols]).astype(BF16)
                acts[b][c, :, cols] = dpre
                wide = dpre.astype(F32)
                acc_b[...] += wide[:, :128] + wide[:, 128:]
        acc_in[...] += sum(jnp.dot(acts[b][c], hs[b][c], preferred_element_type=F32) for c in chunks)

    def backward0(step, carry):
        c = lax.rem(me + n_mem - step, n_mem)

        @pl.when(step > 0)
        def _():
            b_copy(0, c, c).wait_recv()

        backward_chunk(0, c)
        return carry

    def second(i):
        c = lax.rem(jnp.minimum(me, full - 1) + full - i, full)

        @pl.when(c != me)
        def _():
            b_copy(1, c, c).wait_recv()

        return c

    def backward1(step, carry):
        backward_chunk(1, second(2 * step), second(2 * step + 1))
        return carry

    lax.fori_loop(0, CUT_F, forward1, 0)
    mark('waitA0')
    meet(0)
    mark('forward1b')
    lax.fori_loop(CUT_F, n_mem, forward1, 0)
    mark('backward0')
    lax.fori_loop(0, CUT_B, backward0, 0)
    mark('waitA1')

    @pl.when(me < full)
    def _():
        meet(1)

    mark('backward0b')
    lax.fori_loop(CUT_B, n_mem, backward0, 0)
    mark('backward1')
    lax.fori_loop(0, full // 2, backward1, 0)
    for i in range(full // 2 * 2, full):
        backward_chunk(1, second(i))

    def sens_of(*chunks):
        for c in chunks:
            for piece in all_pieces:
                if piece[0] == c:
                    b = piece[1]
                    hs[b][c] = jnp.dot(w_in_t[...], acts[b][c], preferred_element_type=F32).T.astype(BF16)
                    for copy in store_copies(*piece):
                        copy.start()

    mark('gradprep')
    half = hid // 2
    block = half // PARTS
    share = block // plane
    lane = lax.broadcasted_iota(jnp.int32, (hid, 128), 1)
    summed_b = jnp.sum(acc_b[...], axis=1, keepdims=True)
    acc_out[...] = jnp.where(lane == chans, summed_b, acc_out[...])

    def zero_copy(r):
        return pltpu.make_async_remote_copy(
            src_ref=gsend.at[r], dst_ref=c0.at[r], send_sem=send_0.at[r], recv_sem=recv_0.at[r],
            device_id=partner, device_id_type=MESH)

    def one_copy(r, q, slot, dev):
        return pltpu.make_async_remote_copy(
            src_ref=p1.at[r, q], dst_ref=c1.at[r, slot], send_sem=send_1.at[r],
            recv_sem=recv_1.at[r], device_id=dev, device_id_type=MESH)

    def two_copy(r, zz, slot, dev):
        return pltpu.make_async_remote_copy(
            src_ref=z1.at[r], dst_ref=c2.at[r, slot], send_sem=send_2.at[r],
            recv_sem=recv_2.at[r], device_id=dev, device_id_type=MESH)

    def at_fin(r, k, q):
        return (k * PARTS + r) * plane + q

    def three_copy(r, src_q, dst_q, dev):
        return pltpu.make_async_remote_copy(
            src_ref=fin.at[at_fin(r, core, my_q)], dst_ref=fin.at[at_fin(r, core, src_q)],
            send_sem=send_3.at[r], recv_sem=recv_3.at[r],
            device_id=dev, device_id_type=MESH)

    def of_core(r, k):
        return pl.ds(at_fin(r, k, 0), plane)

    def four_copy(r):
        mine = fin.at[of_core(r, core)]
        return pltpu.make_async_remote_copy(
            src_ref=mine, dst_ref=mine, send_sem=send_4.at[r], recv_sem=recv_4.at[r],
            device_id=partner, device_id_type=MESH)

    def fin_out(r, k):
        return pltpu.make_async_copy(fin.at[of_core(r, k)], fin_ref.at[of_core(r, k)], keep.at[0])

    for r in range(PARTS):
        theirs = pl.ds(pl.multiple_of((1 - core) * half + r * block, block), block)
        gsend[r, :, :latent] = acc_in[theirs, :].astype(BF16)
        gsend[r, :, latent:] = acc_out[theirs, :].astype(BF16)
        zero_copy(r).start()
    mark('sens0')
    sens_of(0)
    for r in range(PARTS):
        mark(f'wait0.{r}')
        zero_copy(r).wait_recv()
        mark(f'sum0.{r}')
        mine = pl.ds(pl.multiple_of(core * half + r * block, block), block)
        own[:, :latent] = acc_in[mine, :] + c0[r, :, :latent].astype(F32)
        own[:, latent:] = acc_out[mine, :] + c0[r, :, latent:].astype(F32)
        for q in range(plane):
            p1[r, q] = own[q * share:(q + 1) * share, :].astype(BF16)
        for off in range(1, plane):
            q, dev = plane_dev(off)
            one_copy(r, q, my_q, dev).start()
        c1[r, my_q] = p1[r, my_q]
    mark('sens1')
    sens_of(1, 2, 3)
    for r in range(PARTS):
        mark(f'wait1.{r}')
        took(c1.at[r, pl.ds(0, plane - 1)], recv_1.at[r])
        mark(f'sum1.{r}')
        part = c1[r, 0].astype(F32)
        for q in range(1, plane):
            part = part + c1[r, q].astype(F32)
        z1[r] = part.astype(BF16)
        for off in (4, 3, 5, 2, 6, 1, 7):
            zz, dev = z_dev(off)
            two_copy(r, zz, z, dev).start()
        c2[r, z] = z1[r]
        mark(f'sens2.{r}')
        if r == 0:
            sens_of(4, 5)
        if r == PARTS - 1:
            sens_of(6)
    for r in range(PARTS):
        mark(f'wait2.{r}')
        took(c2.at[r, pl.ds(0, n_z - 1)], recv_2.at[r])
        mark(f'sum2.{r}')
        part = c2[r, 0].astype(F32)
        for zz in range(1, n_z):
            part = part + c2[r, zz].astype(F32)
        fin[at_fin(r, core, my_q)] = part.astype(BF16)
        for off in range(1, plane):
            q, dev = plane_dev(off)
            three_copy(r, my_q, q, dev).start()
        if r == 0:
            sens_of(7)
    for r in range(PARTS):
        mark(f'wait3.{r}')
        took(fin.at[pl.ds(0, plane - 1)], recv_3.at[r])
        four_copy(r).start()
        fin_out(r, core).start()
    for r in range(PARTS):
        mark(f'wait4.{r}')
        took(fin.at[pl.ds(0, plane)], recv_4.at[r])
        fin_out(r, 1 - core).start()
    mark('drain')
    took(sens_ref, store.at[0])
    took(fcast[0].at[pl.ds(0, n_mem - 1)], send_a.at[0])
    took(fpart[0].at[pl.ds(0, n_mem - 1)], send_b.at[0])

    @pl.when(me < full)
    def _():
        took(fcast[1].at[pl.ds(0, full - 1)], send_a.at[1])
        took(fpart[1].at[pl.ds(0, n_mem - 1)], send_b.at[1])

    @pl.when(me == full)
    def _():
        took(fcast[1].at[pl.ds(0, full)], send_a.at[1])

    for r in range(PARTS):
        zero_copy(r).wait_send()
        took(c1.at[r, pl.ds(0, plane - 1)], send_1.at[r])
        took(c2.at[r, pl.ds(0, n_z - 1)], send_2.at[r])
        took(fin.at[pl.ds(0, plane - 1)], send_3.at[r])
        took(fin.at[pl.ds(0, plane)], send_4.at[r])
    took(fin_ref, keep.at[0])
    mark(None)


def finish(geo, sens_ref, fin_ref, out_ref, gin_ref, gout_ref, gb_ref, held, fin, gin, gout, gb, come, go):
    scale, latent, chans = geo
    n = held.shape[0]
    rows = held.shape[2]
    mem = held.shape[1]

    def come_in(i, m):
        return pltpu.make_async_copy(sens_ref.at[m, pl.ds(i * rows, rows), :], held.at[i, m], come.at[mem * i + m])

    def go_out(i, m):
        return pltpu.make_async_copy(held.at[i, m], out_ref.at[m, pl.ds(i * rows, rows), :], go.at[mem * i + m])

    fin_in = pltpu.make_async_copy(fin_ref, fin, come.at[mem * n])
    gin_out = pltpu.make_async_copy(gin, gin_ref, go.at[mem * n])
    gout_out = pltpu.make_async_copy(gout, gout_ref, go.at[mem * n + 1])
    gb_out = pltpu.make_async_copy(gb, gb_ref, go.at[mem * n + 2])
    fin_in.start()
    both = [(i, m) for i in range(n) for m in range(mem)]
    for i, m in both:
        come_in(i, m).start()
    fin_in.wait()
    share = fin.shape[1]
    for r in range(fin.shape[0]):
        gin[r * share:(r + 1) * share, :] = fin[r, :, :latent].astype(F32) * scale
    gin_out.start()
    flipped = fin[:, :, latent:].astype(F32).reshape(gin.shape[0], -1).T * scale
    gout[...] = flipped[:chans, :]
    gb[...] = flipped[chans:chans + 1, :]
    gout_out.start()
    gb_out.start()
    for i, m in both:
        come_in(i, m).wait()
        go_out(i, m).start()
    for i, m in both:
        go_out(i, m).wait()
    gin_out.wait()
    gout_out.wait()
    gb_out.wait()


def on_device(hidden_codes, w_in, b_in, w_out, b_out, target, band_start):
    mem, latent, cells = hidden_codes.shape
    hid = w_in.shape[0]
    chans = w_out.shape[0]
    rows = cells // LON
    n_mem = lax.axis_size("member")
    n_space = lax.axis_size("space")
    n_z = n_space // 4
    plane = 2 * n_mem
    wide = latent + 128
    half = hid // 2
    block = half // PARTS
    share = block // plane
    vm = pl.BlockSpec(memory_space=pltpu.VMEM)
    hbm = pl.BlockSpec(memory_space=pl.ANY)
    dma = pltpu.SemaphoreType.DMA

    def by_sub(make):
        return [make(2 * size) for size in SUBS]

    sens, fin = pl.pallas_call(
        functools.partial(kernel, (n_mem, n_z, cells, rows * n_space)),
        out_shape=(
            jax.ShapeDtypeStruct((mem, cells, latent), BF16),
            jax.ShapeDtypeStruct((2 * PARTS * plane, share, wide), BF16),
        ),
        in_specs=[pl.BlockSpec(memory_space=pltpu.SMEM), hbm] + [vm] * 5,
        out_specs=(hbm, hbm),
        scratch_shapes=[
            *by_sub(lambda n: pltpu.VMEM((n_mem, n, latent), BF16)),
            *by_sub(lambda n: pltpu.VMEM((n_mem, hid, n), F32)),
            *by_sub(lambda n: pltpu.VMEM((n_mem, hid, n), BF16)),
            *by_sub(lambda n: pltpu.VMEM((n_mem, chans, n), BF16)),
            *by_sub(lambda n: pltpu.VMEM((n_mem, chans, n), BF16)),
            *by_sub(lambda n: pltpu.VMEM((n_mem, chans, n), BF16)),
            pltpu.VMEM((8, CHUNK), F32),
            pltpu.VMEM((hid, latent), BF16),
            pltpu.VMEM((latent, hid), BF16),
            pltpu.VMEM((hid, chans), BF16),
            pltpu.VMEM((hid, 128), F32),
            pltpu.VMEM((chans, 128), F32),
            pltpu.VMEM((n_mem, chans, CHUNK), F32),
            pltpu.VMEM((2 * n_mem, chans, CHUNK), F32),
            pltpu.VMEM((hid, latent), F32),
            pltpu.VMEM((hid, 128), F32),
            pltpu.VMEM((hid, 128), F32),
            pltpu.VMEM((PARTS, block, wide), BF16),
            pltpu.VMEM((PARTS, block, wide), BF16),
            pltpu.VMEM((block, wide), F32),
            pltpu.VMEM((PARTS, plane, share, wide), BF16),
            pltpu.VMEM((PARTS, plane, share, wide), BF16),
            pltpu.VMEM((PARTS, share, wide), BF16),
            pltpu.VMEM((PARTS, n_z, share, wide), BF16),
            pltpu.VMEM((2 * PARTS * plane, share, wide), BF16),
            dma((2,)), dma((2,)), dma((2,)), dma((2 * n_mem,)),
            *[dma((PARTS,))] * 10,
            dma((2 * n_mem,)), dma((1,)), dma((1,)),
        ],
        compiler_params=pltpu.CompilerParams(
            collective_id=0, has_side_effects=True, vmem_limit_bytes=67043328),
    )(band_start, jnp.swapaxes(hidden_codes, 1, 2), w_in, b_in.reshape(1, hid), w_out, b_out.reshape(1, chans), target)
    pieces = 6
    sens, gin, gout, gb = pl.pallas_call(
        functools.partial(finish, (1.0 / math.sqrt(2 * n_mem * cells), latent, chans)),
        out_shape=(
            jax.ShapeDtypeStruct((mem, cells, latent), BF16),
            jax.ShapeDtypeStruct((hid, latent), F32),
            jax.ShapeDtypeStruct((chans, hid), F32),
            jax.ShapeDtypeStruct((1, hid), F32),
        ),
        in_specs=[hbm, hbm],
        out_specs=(hbm, hbm, hbm, hbm),
        scratch_shapes=[
            pltpu.VMEM((pieces, mem, cells // pieces, latent), BF16),
            pltpu.VMEM((2 * PARTS * plane, share, wide), BF16),
            pltpu.VMEM((hid, latent), F32),
            pltpu.VMEM((chans, hid), F32),
            pltpu.VMEM((1, hid), F32),
            dma((pieces * mem + 1,)), dma((pieces * mem + 3,)),
        ],
    )(sens, fin)
    return jnp.swapaxes(sens, 1, 2), gin, gout, gb.reshape(hid)


def solution(mesh):
    in_specs = (P("member", None, "space"), P(), P(), P(), P(), P(None, "space"), P("space"))
    out_specs = (P("member", None, "space"), P(), P(), P())
    return jax.shard_map(
        on_device, mesh=mesh, in_specs=in_specs, out_specs=out_specs, check_vma=False
    )
```

```python
import functools
import math

import jax
import jax.numpy as jnp
from jax import lax
from jax.experimental import pallas as pl
from jax.experimental.pallas import tpu as pltpu
from jax.sharding import PartitionSpec as P

LON = 1440
SUBS = (256, 128)
CHUNK = sum(SUBS)
PARTS = 4
LATE = 3
CUT_F = 8
CUT_B = 1
MESH = pl.DeviceIdType.MESH
K0 = math.sqrt(2.0 / math.pi)
K1 = K0 * 0.044715
F32 = jnp.float32
BF16 = jnp.bfloat16


class Mark:
    def __init__(self):
        self.cm = None

    def __call__(self, name):
        if self.cm is not None:
            self.cm.__exit__(None, None, None)
            self.cm = None
        if name:
            self.cm = jax.named_scope(name)
            self.cm.__enter__()


def kernel(
    geo,
    band_ref, h_ref, w_in_ref, b_in_ref, w_out_ref, b_out_ref, target_ref,
    sens_ref, fin_ref,
    hs0, hs1, slopes0, slopes1, acts0, acts1, fcast0, fcast1, fpart0, fpart1, dback0, dback1,
    areas, w_half, w_in_t, w_out_t, bias, bias_out, goal, ftile,
    acc_in, acc_out, acc_b, gsend, c0, own, p1, c1, z1, c2, fin,
    send_a, recv_a, send_b, recv_b, send_0, recv_0, send_1, recv_1, send_2, recv_2, send_3, recv_3, send_4, recv_4,
    load, store, keep,
):
    n_mem, n_z, cells, lat_rows = geo
    hid, latent = w_in_ref.shape
    chans = w_out_ref.shape[0]
    hs, slopes, acts = (hs0, hs1), (slopes0, slopes1), (acts0, acts1)
    fcast, fpart, dback = (fcast0, fcast1), (fpart0, fpart1), (dback0, dback1)
    me = lax.axis_index("member")
    sp = lax.axis_index("space")
    core = lax.rem(sp, 2)
    x_hi = lax.rem(lax.div(sp, 2), 2)
    z = lax.div(sp, 4)
    plane = 2 * n_mem
    my_q = me * 2 + x_hi
    full = cells // CHUNK
    rest = cells - full * CHUNK
    first_at = (0, SUBS[0])

    def plane_dev(off):
        q = lax.rem(my_q + off, plane)
        return q, {"member": lax.div(q, 2), "space": z * 4 + lax.rem(q, 2) * 2 + core}

    def z_dev(off):
        zz = lax.rem(z + off, n_z)
        return zz, {"space": zz * 4 + x_hi * 2 + core}

    partner = {"space": sp + 1 - 2 * core}
    mark = Mark()
    mark('entry')

    def pieces(c, b, size):
        return [(m, pl.ds(c * CHUNK + first_at[b], size), pl.ds(m * SUBS[b], size)) for m in range(2)]

    def load_copies(c, b, size):
        return [
            pltpu.make_async_copy(h_ref.at[m, far, :], hs[b].at[c, near, :], load.at[b * n_mem + c])
            for m, far, near in pieces(c, b, size)]

    def store_copies(c, b, size):
        return [
            pltpu.make_async_copy(hs[b].at[c, near, :], sens_ref.at[m, far, :], store.at[0])
            for m, far, near in pieces(c, b, size)]

    def load_wait(c, b, size):
        pltpu.make_async_copy(
            h_ref.at[0, pl.ds(0, 2 * size), :], hs[b].at[c, pl.ds(0, 2 * size), :], load.at[b * n_mem + c]).wait()

    all_pieces = [(c, 0, SUBS[0] if c < full else rest) for c in range(n_mem)] + [(c, 1, SUBS[1]) for c in range(full)]
    for piece in all_pieces:
        for copy in load_copies(*piece):
            copy.start()

    barrier = pltpu.get_barrier_semaphore()
    for off in range(1, plane):
        pl.semaphore_signal(barrier, inc=1, device_id=plane_dev(off)[1], device_id_type=MESH)
    for off in range(1, n_z):
        pl.semaphore_signal(barrier, inc=1, device_id=z_dev(off)[1], device_id_type=MESH)
    pl.semaphore_signal(barrier, inc=1, device_id=partner, device_id_type=MESH)

    mark('prep')
    for m in range(2):
        hs0[full, m * SUBS[0] + rest:(m + 1) * SUBS[0], :] = jnp.zeros((SUBS[0] - rest, latent), BF16)
    for c in range(n_mem):
        if c < full:
            goal[c] = target_ref[:, c * CHUNK:(c + 1) * CHUNK].astype(F32)
        else:
            goal[c] = jnp.concatenate(
                [target_ref[:, c * CHUNK:cells].astype(F32), jnp.zeros((chans, CHUNK - rest), F32)], axis=1)
    w_in_t[...] = w_in_ref[...].T
    cell = me * CHUNK + lax.broadcasted_iota(jnp.int32, (8, CHUNK), 1)
    row = band_ref[0] + jnp.where(cell < LON, 0, 1)
    angle = (row.astype(F32) + 0.5) * (math.pi / lat_rows) - math.pi / 2
    areas[...] = jnp.where(cell < cells, jnp.cos(angle), 0.0)
    w_half[...] = w_in_ref[...] * 0.5
    w_out_t[...] = w_out_ref[...].T * 0.5
    bias[...] = jnp.broadcast_to(0.5 * b_in_ref[...], (128, hid)).T
    bias_out[...] = jnp.broadcast_to(b_out_ref[...], (128, chans)).T
    acc_in[...] = jnp.zeros_like(acc_in)
    acc_out[...] = jnp.zeros_like(acc_out)
    acc_b[...] = jnp.zeros_like(acc_b)

    def a_copy(b, d, slot):
        return pltpu.make_async_remote_copy(
            src_ref=fcast[b].at[d], dst_ref=fpart[b].at[slot], send_sem=send_a.at[b],
            recv_sem=recv_a.at[b], device_id={"member": d}, device_id_type=MESH)

    def b_piece(b, d, piece):
        return pltpu.make_async_remote_copy(
            src_ref=fpart[b].at[d, piece, :], dst_ref=dback[b].at[me, piece, :], send_sem=send_b.at[b],
            recv_sem=recv_b.at[b * n_mem + me], device_id={"member": d}, device_id_type=MESH)

    def b_copy(b, d, slot):
        return pltpu.make_async_remote_copy(
            src_ref=fpart[b].at[d], dst_ref=dback[b].at[slot], send_sem=send_b.at[b],
            recv_sem=recv_b.at[b * n_mem + slot], device_id={"member": d}, device_id_type=MESH)

    def took(ref, sem):
        pltpu.make_async_copy(ref, ref, sem).wait()

    def forward_chunk(b, c):
        b2 = jnp.concatenate([bias[...]] * 2, axis=1)
        bo2 = jnp.concatenate([bias_out[...]] * 2, axis=1)
        for j in range(2 * SUBS[b] // 256):
            cols = slice(j * 256, (j + 1) * 256)
            x = lax.dot_general(
                w_half[...], hs[b][c, cols, :], (((1,), (1,)), ((), ())), preferred_element_type=F32) + b2
            poly = 2.0 * K0 + (8.0 * K1) * (x * x)
            t = jnp.tanh(x * poly)
            p = 1.0 + t
            a = x * p
            slopes[b][c, :, cols] = p + (a * (1.0 - t)) * (3.0 * poly - 4.0 * K0)
            a = a.astype(BF16)
            acts[b][c, :, cols] = a
            fcast[b][c, :, cols] = (jnp.dot(w_out_ref[...], a, preferred_element_type=F32) + bo2).astype(BF16)

    mark('forward0')

    def forward0(step, carry):
        c = lax.rem(me + 1 + step, n_mem)

        @pl.when(c < full)
        def _():
            load_wait(c, 0, SUBS[0])

        @pl.when(c == full)
        def _():
            load_wait(c, 0, rest)

        forward_chunk(0, c)

        @pl.when(step == LATE)
        def _():
            pl.semaphore_wait(barrier, plane - 1 + n_z - 1 + 1)
            for early in range(LATE):
                a_copy(0, lax.rem(me + 1 + early, n_mem), me).start()

        @pl.when((step >= LATE) & (step < n_mem - 1))
        def _():
            a_copy(0, c, me).start()

        return carry

    lax.fori_loop(0, n_mem, forward0, 0)
    mark('forward1')

    def forward1(step, carry):
        c = lax.rem(me + 1 + step, n_mem)

        @pl.when(c < full)
        def _():
            load_wait(c, 1, SUBS[1])
            forward_chunk(1, c)

            @pl.when(step < n_mem - 1)
            def _():
                a_copy(1, c, me).start()

        return carry


    def meet(b):
        size = SUBS[b]
        at = first_at[b]
        fpart[b][me] = fcast[b][me]
        took(fpart[b].at[pl.ds(0, n_mem - 1)], recv_a.at[b])
        if b == 0:
            mark('pairs0')
        for p in range(n_mem):
            for m in range(2):
                ftile[2 * p + m, :, at:at + size] = fpart[b][p, :, m * size:(m + 1) * size].astype(F32)

        def pairs(r, carry):
            rows = pl.ds(pl.multiple_of(r * 8, 8), 8)
            for k in range(size // 128):
                cols = slice(at + k * 128, at + (k + 1) * 128)
                area = areas[:, cols]
                f = [ftile[i, rows, cols] for i in range(2 * n_mem)]
                total = [None] * (2 * n_mem)
                for i in range(2 * n_mem):
                    for j in range(i + 1, 2 * n_mem):
                        d = f[i] - f[j]
                        v = d * lax.rsqrt(d * d + 0.0625)
                        total[i] = v if total[i] is None else total[i] + v
                        total[j] = -v if total[j] is None else total[j] - v
                g = goal[me, rows, cols]
                for i in range(2 * n_mem):
                    d = f[i] - g
                    v = d * lax.rsqrt(d * d + 0.0625)
                    ftile[i, rows, cols] = area * (v - total[i] * (1.0 / (2 * n_mem)))
            return carry

        lo = 0
        for hi in (chans // 16 * 8, chans):
            lax.fori_loop(lo // 8, hi // 8, pairs, 0)
            piece = slice(lo, hi)
            for p in range(n_mem):
                for m in range(2):
                    fpart[b][p, piece, m * size:(m + 1) * size] = ftile[2 * p + m, piece, at:at + size].astype(BF16)
            for off in range(1, n_mem):
                b_piece(b, lax.rem(me + off, n_mem), pl.ds(lo, hi - lo)).start()
            lo = hi
        dback[b][me] = fpart[b][me]

    def backward_chunk(b, *chunks):
        acc_out[:, :chans] += sum(
            lax.dot_general(acts[b][c], dback[b][c], (((1,), (1,)), ((), ())), preferred_element_type=F32)
            for c in chunks)
        for c in chunks:
            for j in range(2 * SUBS[b] // 256):
                cols = slice(j * 256, (j + 1) * 256)
                dact = jnp.dot(w_out_t[...], dback[b][c, :, cols], preferred_element_type=F32)
                dpre = (dact * slopes[b][c, :, cols]).astype(BF16)
                acts[b][c, :, cols] = dpre
                wide = dpre.astype(F32)
                acc_b[...] += wide[:, :128] + wide[:, 128:]
        acc_in[...] += sum(jnp.dot(acts[b][c], hs[b][c], preferred_element_type=F32) for c in chunks)

    def backward0(step, carry):
        c = lax.rem(me + n_mem - step, n_mem)

        @pl.when(step > 0)
        def _():
            b_copy(0, c, c).wait_recv()

        backward_chunk(0, c)
        return carry

    def second(i):
        c = lax.rem(jnp.minimum(me, full - 1) + full - i, full)

        @pl.when(c != me)
        def _():
            b_copy(1, c, c).wait_recv()

        return c

    def backward1(step, carry):
        backward_chunk(1, second(2 * step + 1), second(2 * step + 2))
        return carry

    lax.fori_loop(0, CUT_F, forward1, 0)
    mark('waitA0')
    meet(0)
    mark('forward1b')
    lax.fori_loop(CUT_F, n_mem, forward1, 0)
    mark('backward0')
    lax.fori_loop(0, CUT_B, backward0, 0)
    mark('waitA1')

    @pl.when(me < full)
    def _():
        meet(1)

    @pl.when(me < full)
    def _():
        backward_chunk(1, me)

    mark('backward0b')
    lax.fori_loop(CUT_B, n_mem, backward0, 0)
    mark('backward1')
    lax.fori_loop(0, (full - 1) // 2, backward1, 0)

    @pl.when(me == full)
    def _():
        backward_chunk(1, second(0))

    def sens_of(*chunks):
        for c in chunks:
            for piece in all_pieces:
                if piece[0] == c:
                    b = piece[1]
                    hs[b][c] = jnp.dot(w_in_t[...], acts[b][c], preferred_element_type=F32).T.astype(BF16)
                    for copy in store_copies(*piece):
                        copy.start()

    mark('gradprep')
    half = hid // 2
    block = half // PARTS
    share = block // plane
    lane = lax.broadcasted_iota(jnp.int32, (hid, 128), 1)
    summed_b = jnp.sum(acc_b[...], axis=1, keepdims=True)
    acc_out[...] = jnp.where(lane == chans, summed_b, acc_out[...])

    def zero_copy(r):
        return pltpu.make_async_remote_copy(
            src_ref=gsend.at[r], dst_ref=c0.at[r], send_sem=send_0.at[r], recv_sem=recv_0.at[r],
            device_id=partner, device_id_type=MESH)

    def one_copy(r, q, slot, dev):
        return pltpu.make_async_remote_copy(
            src_ref=p1.at[r, q], dst_ref=c1.at[r, slot], send_sem=send_1.at[r],
            recv_sem=recv_1.at[r], device_id=dev, device_id_type=MESH)

    def two_copy(r, zz, slot, dev):
        return pltpu.make_async_remote_copy(
            src_ref=z1.at[r], dst_ref=c2.at[r, slot], send_sem=send_2.at[r],
            recv_sem=recv_2.at[r], device_id=dev, device_id_type=MESH)

    def at_fin(r, k, q):
        return (k * PARTS + r) * plane + q

    def three_copy(r, src_q, dst_q, dev):
        return pltpu.make_async_remote_copy(
            src_ref=fin.at[at_fin(r, core, my_q)], dst_ref=fin.at[at_fin(r, core, src_q)],
            send_sem=send_3.at[r], recv_sem=recv_3.at[r],
            device_id=dev, device_id_type=MESH)

    def of_core(r, k):
        return pl.ds(at_fin(r, k, 0), plane)

    def four_copy(r):
        mine = fin.at[of_core(r, core)]
        return pltpu.make_async_remote_copy(
            src_ref=mine, dst_ref=mine, send_sem=send_4.at[r], recv_sem=recv_4.at[r],
            device_id=partner, device_id_type=MESH)

    def fin_out(r, k):
        return pltpu.make_async_copy(fin.at[of_core(r, k)], fin_ref.at[of_core(r, k)], keep.at[0])

    for r in range(PARTS):
        theirs = pl.ds(pl.multiple_of((1 - core) * half + r * block, block), block)
        gsend[r, :, :latent] = acc_in[theirs, :].astype(BF16)
        gsend[r, :, latent:] = acc_out[theirs, :].astype(BF16)
        zero_copy(r).start()
    mark('sens0')
    sens_of(0)
    for r in range(PARTS):
        mark(f'wait0.{r}')
        zero_copy(r).wait_recv()
        mark(f'sum0.{r}')
        mine = pl.ds(pl.multiple_of(core * half + r * block, block), block)
        own[:, :latent] = acc_in[mine, :] + c0[r, :, :latent].astype(F32)
        own[:, latent:] = acc_out[mine, :] + c0[r, :, latent:].astype(F32)
        for q in range(plane):
            p1[r, q] = own[q * share:(q + 1) * share, :].astype(BF16)
        for off in range(1, plane):
            q, dev = plane_dev(off)
            one_copy(r, q, my_q, dev).start()
        c1[r, my_q] = p1[r, my_q]
    mark('sens1')
    sens_of(1, 2, 3)
    for r in range(PARTS):
        mark(f'wait1.{r}')
        took(c1.at[r, pl.ds(0, plane - 1)], recv_1.at[r])
        mark(f'sum1.{r}')
        part = c1[r, 0].astype(F32)
        for q in range(1, plane):
            part = part + c1[r, q].astype(F32)
        z1[r] = part.astype(BF16)
        for off in (4, 3, 5, 2, 6, 1, 7):
            zz, dev = z_dev(off)
            two_copy(r, zz, z, dev).start()
        c2[r, z] = z1[r]
        mark(f'sens2.{r}')
        if r == 0:
            sens_of(4, 5)
        if r == PARTS - 1:
            sens_of(6)
    for r in range(PARTS):
        mark(f'wait2.{r}')
        took(c2.at[r, pl.ds(0, n_z - 1)], recv_2.at[r])
        mark(f'sum2.{r}')
        part = c2[r, 0].astype(F32)
        for zz in range(1, n_z):
            part = part + c2[r, zz].astype(F32)
        fin[at_fin(r, core, my_q)] = part.astype(BF16)
        for off in range(1, plane):
            q, dev = plane_dev(off)
            three_copy(r, my_q, q, dev).start()
        if r == 0:
            sens_of(7)
    for r in range(PARTS):
        mark(f'wait3.{r}')
        took(fin.at[pl.ds(0, plane - 1)], recv_3.at[r])
        four_copy(r).start()
        fin_out(r, core).start()
    for r in range(PARTS):
        mark(f'wait4.{r}')
        took(fin.at[pl.ds(0, plane)], recv_4.at[r])
        fin_out(r, 1 - core).start()
    mark('drain')
    took(sens_ref, store.at[0])
    took(fcast[0].at[pl.ds(0, n_mem - 1)], send_a.at[0])
    took(fpart[0].at[pl.ds(0, n_mem - 1)], send_b.at[0])

    @pl.when(me < full)
    def _():
        took(fcast[1].at[pl.ds(0, full - 1)], send_a.at[1])
        took(fpart[1].at[pl.ds(0, n_mem - 1)], send_b.at[1])

    @pl.when(me == full)
    def _():
        took(fcast[1].at[pl.ds(0, full)], send_a.at[1])

    for r in range(PARTS):
        zero_copy(r).wait_send()
        took(c1.at[r, pl.ds(0, plane - 1)], send_1.at[r])
        took(c2.at[r, pl.ds(0, n_z - 1)], send_2.at[r])
        took(fin.at[pl.ds(0, plane - 1)], send_3.at[r])
        took(fin.at[pl.ds(0, plane)], send_4.at[r])
    took(fin_ref, keep.at[0])
    mark(None)


def finish(geo, sens_ref, fin_ref, out_ref, gin_ref, gout_ref, gb_ref, held, fin, gin, gout, gb, come, go):
    scale, latent, chans = geo
    n = held.shape[0]
    rows = held.shape[2]
    mem = held.shape[1]

    def come_in(i, m):
        return pltpu.make_async_copy(sens_ref.at[m, pl.ds(i * rows, rows), :], held.at[i, m], come.at[mem * i + m])

    def go_out(i, m):
        return pltpu.make_async_copy(held.at[i, m], out_ref.at[m, pl.ds(i * rows, rows), :], go.at[mem * i + m])

    fin_in = pltpu.make_async_copy(fin_ref, fin, come.at[mem * n])
    gin_out = pltpu.make_async_copy(gin, gin_ref, go.at[mem * n])
    gout_out = pltpu.make_async_copy(gout, gout_ref, go.at[mem * n + 1])
    gb_out = pltpu.make_async_copy(gb, gb_ref, go.at[mem * n + 2])
    fin_in.start()
    both = [(i, m) for i in range(n) for m in range(mem)]
    for i, m in both:
        come_in(i, m).start()
    fin_in.wait()
    share = fin.shape[1]
    for r in range(fin.shape[0]):
        gin[r * share:(r + 1) * share, :] = fin[r, :, :latent].astype(F32) * scale
    gin_out.start()
    flipped = fin[:, :, latent:].astype(F32).reshape(gin.shape[0], -1).T * scale
    gout[...] = flipped[:chans, :]
    gb[...] = flipped[chans:chans + 1, :]
    gout_out.start()
    gb_out.start()
    for i, m in both:
        come_in(i, m).wait()
        go_out(i, m).start()
    for i, m in both:
        go_out(i, m).wait()
    gin_out.wait()
    gout_out.wait()
    gb_out.wait()


def on_device(hidden_codes, w_in, b_in, w_out, b_out, target, band_start):
    mem, latent, cells = hidden_codes.shape
    hid = w_in.shape[0]
    chans = w_out.shape[0]
    rows = cells // LON
    n_mem = lax.axis_size("member")
    n_space = lax.axis_size("space")
    n_z = n_space // 4
    plane = 2 * n_mem
    wide = latent + 128
    half = hid // 2
    block = half // PARTS
    share = block // plane
    vm = pl.BlockSpec(memory_space=pltpu.VMEM)
    hbm = pl.BlockSpec(memory_space=pl.ANY)
    dma = pltpu.SemaphoreType.DMA

    def by_sub(make):
        return [make(2 * size) for size in SUBS]

    sens, fin = pl.pallas_call(
        functools.partial(kernel, (n_mem, n_z, cells, rows * n_space)),
        out_shape=(
            jax.ShapeDtypeStruct((mem, cells, latent), BF16),
            jax.ShapeDtypeStruct((2 * PARTS * plane, share, wide), BF16),
        ),
        in_specs=[pl.BlockSpec(memory_space=pltpu.SMEM), hbm] + [vm] * 5,
        out_specs=(hbm, hbm),
        scratch_shapes=[
            *by_sub(lambda n: pltpu.VMEM((n_mem, n, latent), BF16)),
            *by_sub(lambda n: pltpu.VMEM((n_mem, hid, n), F32)),
            *by_sub(lambda n: pltpu.VMEM((n_mem, hid, n), BF16)),
            *by_sub(lambda n: pltpu.VMEM((n_mem, chans, n), BF16)),
            *by_sub(lambda n: pltpu.VMEM((n_mem, chans, n), BF16)),
            *by_sub(lambda n: pltpu.VMEM((n_mem, chans, n), BF16)),
            pltpu.VMEM((8, CHUNK), F32),
            pltpu.VMEM((hid, latent), BF16),
            pltpu.VMEM((latent, hid), BF16),
            pltpu.VMEM((hid, chans), BF16),
            pltpu.VMEM((hid, 128), F32),
            pltpu.VMEM((chans, 128), F32),
            pltpu.VMEM((n_mem, chans, CHUNK), F32),
            pltpu.VMEM((2 * n_mem, chans, CHUNK), F32),
            pltpu.VMEM((hid, latent), F32),
            pltpu.VMEM((hid, 128), F32),
            pltpu.VMEM((hid, 128), F32),
            pltpu.VMEM((PARTS, block, wide), BF16),
            pltpu.VMEM((PARTS, block, wide), BF16),
            pltpu.VMEM((block, wide), F32),
            pltpu.VMEM((PARTS, plane, share, wide), BF16),
            pltpu.VMEM((PARTS, plane, share, wide), BF16),
            pltpu.VMEM((PARTS, share, wide), BF16),
            pltpu.VMEM((PARTS, n_z, share, wide), BF16),
            pltpu.VMEM((2 * PARTS * plane, share, wide), BF16),
            dma((2,)), dma((2,)), dma((2,)), dma((2 * n_mem,)),
            *[dma((PARTS,))] * 10,
            dma((2 * n_mem,)), dma((1,)), dma((1,)),
        ],
        compiler_params=pltpu.CompilerParams(
            collective_id=0, has_side_effects=True, vmem_limit_bytes=67043328),
    )(band_start, jnp.swapaxes(hidden_codes, 1, 2), w_in, b_in.reshape(1, hid), w_out, b_out.reshape(1, chans), target)
    pieces = 6
    sens, gin, gout, gb = pl.pallas_call(
        functools.partial(finish, (1.0 / math.sqrt(2 * n_mem * cells), latent, chans)),
        out_shape=(
            jax.ShapeDtypeStruct((mem, cells, latent), BF16),
            jax.ShapeDtypeStruct((hid, latent), F32),
            jax.ShapeDtypeStruct((chans, hid), F32),
            jax.ShapeDtypeStruct((1, hid), F32),
        ),
        in_specs=[hbm, hbm],
        out_specs=(hbm, hbm, hbm, hbm),
        scratch_shapes=[
            pltpu.VMEM((pieces, mem, cells // pieces, latent), BF16),
            pltpu.VMEM((2 * PARTS * plane, share, wide), BF16),
            pltpu.VMEM((hid, latent), F32),
            pltpu.VMEM((chans, hid), F32),
            pltpu.VMEM((1, hid), F32),
            dma((pieces * mem + 1,)), dma((pieces * mem + 3,)),
        ],
    )(sens, fin)
    return jnp.swapaxes(sens, 1, 2), gin, gout, gb.reshape(hid)


def solution(mesh):
    in_specs = (P("member", None, "space"), P(), P(), P(), P(), P(None, "space"), P("space"))
    out_specs = (P("member", None, "space"), P(), P(), P())
    return jax.shard_map(
        on_device, mesh=mesh, in_specs=in_specs, out_specs=out_specs, check_vma=False
    )
```
